32 devices in a mesh: dp: 8 (over z, x), mp: 4 (over y, core).
Axes of the slice: x: 2, y: 2, z: 4, core: 2. Of those that a mesh axis runs over, the one named last changes fastest.
Arguments:
- partials: bfloat16 [8, 256, 8192], P('dp', None, 'mp'), may hold values from -11 to 11
- momentum: float32 [32, 256, 256], P(('dp', 'mp')), may hold values from -0.3 to 0.3
- second: float32 [32, 256, 256], P(('dp', 'mp')), may hold values from 0.0002 to 0.02
- left_stat: float32 [32, 256, 256], P(('dp', 'mp')), may hold values from -36 to 36.5, as said below
- right_stat: float32 [32, 256, 256], P(('dp', 'mp')), may hold values from -36 to 36.5, as said below
- left_basis: float32 [32, 256, 256], P(('dp', 'mp')), may hold values from -1 to 1, as said below
- right_basis: float32 [32, 256, 256], P(('dp', 'mp')), may hold values from -1 to 1, as said below
Outputs:
- update: bfloat16 [256, 8192], P(None, 'mp')
- momentum_new: float32 [32, 256, 256], P(('dp', 'mp'))
- second_new: float32 [32, 256, 256], P(('dp', 'mp'))
- left_new: float32 [32, 256, 256], P(('dp', 'mp'))
- right_new: float32 [32, 256, 256], P(('dp', 'mp'))
- left_basis_new: float32 [32, 256, 256], P(('dp', 'mp'))
- right_basis_new: float32 [32, 256, 256], P(('dp', 'mp'))
The draws below stay inside these ranges and needn't reach their ends.
Inputs may be any that keep to these rules, and one draw needn't show every extreme that they name: `left_stat`: each block is symmetric positive definite. `right_stat`: each block is symmetric positive definite. `left_basis`: each block is an orthogonal matrix. `right_basis`: each block is an orthogonal matrix.
All inputs are finite; a program needn't handle non-finite values.
Results may differ from the reference program's by a relative error of at most 0.00045.
Values may be sent and summed in bfloat16 or wider, within the bound.
No kernel may reach another device: no remote copies, remote signals or barrier semaphores. Data moves between devices by JAX's collectives and lax.ppermute only.
A program may use at most 128 MiB of HBM per device.

```python
import math
import jax
import jax.numpy as jnp
from jax import lax

D = 8192
BLOCK = 256
TILES_DEV = 1
REPLICAS = 8
ROWS = 256
TILES = 32
N_DP = 8
N_MP = 4


def draw_partials(key, part):
    keys = jax.random.split(jax.random.fold_in(key, 7), 4)
    row_scale = jnp.exp(jax.random.uniform(keys[0], (ROWS, 1), jnp.float32, 0.0, math.log(10.0)))
    col_scale = jnp.exp(jax.random.uniform(keys[1], (1, D), jnp.float32, 0.0, math.log(10.0)))
    position = jnp.arange(ROWS, dtype=jnp.float32)[:, None] / ROWS
    rise = 3.0 ** position
    noise = jnp.clip(jax.random.normal(keys[3], (REPLICAS, ROWS, D), jnp.float32), -6.0, 6.0)
    scale = 0.001 / math.sqrt(REPLICAS)
    return (scale * rise * row_scale * col_scale * noise).astype(jnp.bfloat16)


def spd_blocks(key):
    factor = jnp.clip(jax.random.normal(key, (TILES, BLOCK, BLOCK), jnp.float32), -6.0, 6.0)
    gram = jnp.einsum('tij,tkj->tik', factor, factor, precision=jax.lax.Precision.HIGHEST) / BLOCK
    return gram + 0.5 * jnp.eye(BLOCK, dtype=jnp.float32)[None]


def draw_left_stat(key, part):
    return spd_blocks(jax.random.fold_in(key, 11))


def draw_right_stat(key, part):
    return spd_blocks(jax.random.fold_in(key, 12))


def orthogonal_blocks(key):
    factor = jax.random.normal(key, (TILES, BLOCK, BLOCK), jnp.float32)
    basis, unused = jnp.linalg.qr(factor)
    return jnp.clip(basis, -1.0, 1.0)


def draw_left_basis(key, part):
    return orthogonal_blocks(jax.random.fold_in(key, 13))


def draw_right_basis(key, part):
    return orthogonal_blocks(jax.random.fold_in(key, 14))


def steps_of(own_key, extent, cuts, low, largest):
    gain = 1.0
    for axis_at, blocks in cuts:
        draws = jax.random.uniform(jax.random.fold_in(jax.random.fold_in(own_key, 6), axis_at), (blocks,), jnp.float32, low / len(cuts), largest / len(cuts))
        gain = gain * jnp.repeat(jnp.exp(draws), extent[axis_at] // blocks).reshape((-1,) + (1,) * (len(extent) - 1 - axis_at))
    return gain


def normal_values(own_key, extent, spread, limit, shards=(), held_as=jnp.bfloat16):
    level = steps_of(own_key, extent, shards, -0.22, 0.18) if shards else 1.0
    result = jax.random.normal(own_key, extent, jnp.float32) * spread * level
    return jnp.minimum(jnp.maximum(result, -limit), limit).astype(held_as)


def setup_inputs(seed: int = 0) -> dict:
    arg_keys = jax.random.split(jax.random.key(seed), 8)
    partials = draw_partials(jax.random.fold_in(arg_keys[7], 71), 0)
    momentum = normal_values(arg_keys[1], (TILES, BLOCK, BLOCK), 0.05, 0.3, ((0, 32),), jnp.float32)
    second = jnp.clip(jnp.exp(math.log(0.02) - 4.6051702 * jax.random.uniform(arg_keys[2], (TILES, BLOCK, BLOCK), jnp.float32) ** steps_of(arg_keys[2], (TILES, BLOCK, BLOCK), ((0, 32),), -0.2, 0.2)), 0.0002, 0.02)
    left_stat = draw_left_stat(jax.random.fold_in(arg_keys[7], 71), 0)
    right_stat = draw_right_stat(jax.random.fold_in(arg_keys[7], 71), 0)
    left_basis = draw_left_basis(jax.random.fold_in(arg_keys[7], 71), 0)
    right_basis = draw_right_basis(jax.random.fold_in(arg_keys[7], 71), 0)
    return {"partials": partials, "momentum": momentum, "second": second, "left_stat": left_stat, "right_stat": right_stat, "left_basis": left_basis, "right_basis": right_basis}


beta_first = 0.9
beta_second = 0.95
epsilon = 1e-08
highest = lax.Precision.HIGHEST

def product(left, right):
    return jnp.einsum('tij,tjk->tik', left, right, precision=highest)

def inner_left(left, right):
    return jnp.einsum('tji,tjk->tik', left, right, precision=highest)

def outer_right(left, right):
    return jnp.einsum('tij,tkj->tik', left, right, precision=highest)

def refresh(statistic, basis):
    powered = product(statistic, basis)
    factor = jnp.linalg.cholesky(inner_left(powered, powered))
    return lax.linalg.triangular_solve(factor, powered, left_side=False, lower=True, transpose_a=True)

def to_blocks(matrix):
    row_bands = ROWS // BLOCK
    col_bands = D // (BLOCK * N_MP)
    stacked = matrix.reshape(row_bands, BLOCK, N_MP, col_bands, BLOCK)
    stacked = jnp.transpose(stacked, (2, 0, 3, 1, 4)).reshape(N_MP, N_DP, TILES_DEV, BLOCK, BLOCK)
    return jnp.transpose(stacked, (1, 0, 2, 3, 4)).reshape(TILES, BLOCK, BLOCK)

def from_blocks(stacked):
    row_bands = ROWS // BLOCK
    col_bands = D // (BLOCK * N_MP)
    grouped = stacked.reshape(N_DP, N_MP, TILES_DEV, BLOCK, BLOCK)
    grouped = jnp.transpose(grouped, (1, 0, 2, 3, 4)).reshape(N_MP, row_bands, col_bands, BLOCK, BLOCK)
    return jnp.transpose(grouped, (1, 3, 0, 2, 4)).reshape(ROWS, D)

def accumulate(running, replica):
    return (running + replica.astype(jnp.float32), None)

def reference(partials, momentum, second, left_stat, right_stat, left_basis, right_basis):
    gradient, unused = lax.scan(accumulate, jnp.zeros((ROWS, D), jnp.float32), partials)
    blocks = to_blocks(gradient)
    grad_norm = jnp.sum(blocks * blocks)
    left_new = beta_second * left_stat + (1.0 - beta_second) * outer_right(blocks, blocks)
    right_new = beta_second * right_stat + (1.0 - beta_second) * inner_left(blocks, blocks)
    momentum_new = beta_first * momentum + (1.0 - beta_first) * blocks
    grad_rot = product(inner_left(left_basis, blocks), right_basis)
    moment_rot = product(inner_left(left_basis, momentum_new), right_basis)
    second_new = beta_second * second + (1.0 - beta_second) * grad_rot * grad_rot
    direction = moment_rot / (jnp.sqrt(second_new) + epsilon)
    step_norm = jnp.sum(direction * direction)
    raw_step = outer_right(product(left_basis, direction), right_basis)
    update = (raw_step * jnp.sqrt(grad_norm / step_norm)).astype(jnp.bfloat16)
    return (from_blocks(update), momentum_new, second_new, left_new, right_new, refresh(left_new, left_basis), refresh(right_new, right_basis))
```

```python
import jax
import jax.numpy as jnp
from jax import lax
from jax.experimental import pallas as pl
from jax.experimental.pallas import tpu as pltpu
from jax.sharding import PartitionSpec as P

beta_first = 0.9
beta_second = 0.95
epsilon = 1e-08
highest = lax.Precision.HIGHEST
SUB = 8
LANES = 128
PANEL = 32


def product(left, right):
    return jnp.einsum("tij,tjk->tik", left, right, precision=highest)


def inner_left(left, right):
    return jnp.einsum("tji,tjk->tik", left, right, precision=highest)


def outer_right(left, right):
    return jnp.einsum("tij,tkj->tik", left, right, precision=highest)


def dot(left, right, left_dim, right_dim):
    return lax.dot_general(
        left,
        right,
        (((left_dim,), (right_dim,)), ((), ())),
        precision=highest,
        preferred_element_type=jnp.float32,
    )


def split(value):
    high = value.astype(jnp.bfloat16)
    rest = value - high.astype(jnp.float32)
    middle = rest.astype(jnp.bfloat16)
    low = (rest - middle.astype(jnp.float32)).astype(jnp.bfloat16)
    return high, middle, low


def lane(value, at):
    return jnp.broadcast_to(value[:, at:at + 1], (SUB, LANES))


def row(value, at):
    return jnp.broadcast_to(value[at:at + 1, :], (SUB, LANES))


def eliminate(work, order, rows):
    tiles = 2 * order // LANES
    groups = PANEL // SUB
    for start in range(0, order, PANEL):
        first = start // LANES
        live = range(first, tiles)
        held = [
            {v: work[start + SUB * h:start + SUB * (h + 1), v * LANES:(v + 1) * LANES] for v in live}
            for h in range(groups)
        ]
        for g in range(groups):
            at = (start + SUB * g) % LANES
            cols = {h: [lane(held[h][first], at + k) for k in range(SUB)] for h in range(g, groups)}
            yield
            for k in range(SUB):
                inverse = lax.rsqrt(row(cols[g][k], k))
                factor = {h: cols[h][k] * inverse for h in range(g, groups)}
                below = jnp.where(rows > k, factor[g], 0.0)
                for l in range(k + 1, SUB):
                    pivot = row(factor[g], l)
                    cols[g][l] = cols[g][l] - below * pivot
                    for h in range(g + 1, groups):
                        cols[h][l] = cols[h][l] - factor[h] * pivot
                for v in live:
                    top = row(held[g][v], k) * inverse
                    held[g][v] = jnp.where(rows == k, top, held[g][v] - below * top)
                    for h in range(g + 1, groups):
                        held[h][v] = held[h][v] - factor[h] * top
                yield
        for h in range(groups):
            for v in live:
                work[start + SUB * h:start + SUB * (h + 1), v * LANES:(v + 1) * LANES] = held[h][v]
        after = start + PANEL
        if after < order:
            base = (after // LANES) * LANES
            high, middle, low = split(work[start:after, base:])
            left = jnp.concatenate([high, high, middle, high, low, middle], axis=0)[:, :order - base]
            right = jnp.concatenate([high, middle, high, low, high, middle], axis=0)
            change = lax.dot_general(
                left, right, (((0,), (0,)), ((), ())), preferred_element_type=jnp.float32
            )
            work[after:, base:] = work[after:, base:] - change[after - base:]
        yield


def refresh_body(left_stat, left_basis, right_stat, right_basis, left_out, right_out, left_work, right_work):
    order = left_stat.shape[0]
    rows = lax.broadcasted_iota(jnp.int32, (SUB, LANES), 0)
    for stat, basis, work in ((left_stat, left_basis, left_work), (right_stat, right_basis, right_work)):
        powered_t = dot(basis[...], stat[...], 0, 0)
        work[:, order:] = powered_t
        work[:, :order] = dot(powered_t, powered_t, 1, 1)
    for _ in zip(eliminate(left_work, order, rows), eliminate(right_work, order, rows)):
        pass
    left_out[...] = left_work[:, order:].T
    right_out[...] = right_work[:, order:].T


def refresh(left_stat, left_basis, right_stat, right_basis):
    order = left_stat.shape[-1]
    result = jax.ShapeDtypeStruct((order, order), jnp.float32)
    return pl.pallas_call(
        refresh_body,
        out_shape=(result, result),
        scratch_shapes=[pltpu.VMEM((order, 2 * order), jnp.float32)] * 2,
        name="refresh",
    )(left_stat, left_basis, right_stat, right_basis)


def partner_pairs(size, step):
    if size & (size - 1):
        return [(at, (at + step) % size) for at in range(size)]
    return [(at, at ^ step) for at in range(size)]


def partner(at, size, step):
    return (at + step) % size if size & (size - 1) else at ^ step


def source(at, size, step):
    return (at - step) % size if size & (size - 1) else at ^ step


def swap(value, axis, size, step):
    return lax.ppermute(value, axis, partner_pairs(size, step))


def all_sum(value, sizes):
    for axis in sizes:
        size = sizes[axis]
        if size & (size - 1):
            value = lax.psum(value, axis)
            continue
        step = 1
        while step < size:
            value = value + swap(value, axis, size, step)
            step *= 2
    return value


def on_device(sizes, partials, momentum, second, left_stat, right_stat, left_basis, right_basis):
    tiles, order = left_basis.shape[:2]
    replicas = sizes["dp"]
    at = lax.axis_index("dp")
    replica_part = partials[0]
    row_count, shard_width = replica_part.shape
    col_bands = shard_width // order

    def corner(number):
        return (number // col_bands) * order, (number % col_bands) * order

    def chunk(owner):
        return jnp.stack([
            lax.dynamic_slice(replica_part, corner(owner * tiles + tile), (order, order))
            for tile in range(tiles)
        ])

    steps = sorted(range(1, replicas), key=lambda step: -step)
    received = [swap(chunk(partner(at, replicas, step)), "dp", replicas, step) for step in steps]
    gradient = chunk(at).astype(jnp.float32)
    for piece in received:
        gradient = gradient + piece.astype(jnp.float32)
    grad_local = jnp.sum(gradient * gradient)
    left_new = beta_second * left_stat + (1.0 - beta_second) * outer_right(gradient, gradient)
    right_new = beta_second * right_stat + (1.0 - beta_second) * inner_left(gradient, gradient)
    momentum_new = beta_first * momentum + (1.0 - beta_first) * gradient
    grad_rot = product(inner_left(left_basis, gradient), right_basis)
    moment_rot = product(inner_left(left_basis, momentum_new), right_basis)
    second_new = beta_second * second + (1.0 - beta_second) * grad_rot * grad_rot
    direction = moment_rot / (jnp.sqrt(second_new) + epsilon)
    step_local = jnp.sum(direction * direction)
    norms = all_sum(jnp.stack([grad_local, step_local]), sizes)
    raw_step = outer_right(product(left_basis, direction), right_basis)
    update = (raw_step * jnp.sqrt(norms[0] / norms[1])).astype(jnp.bfloat16)

    assembled = jnp.zeros((row_count, shard_width), jnp.bfloat16)

    def place(assembled, owner, value):
        for tile in range(tiles):
            assembled = lax.dynamic_update_slice(assembled, value[tile], corner(owner * tiles + tile))
        return assembled

    near = [(0, update)]
    if replicas & (replicas - 1) == 0 and replicas > 1:
        far = replicas // 2
        across = swap(update, "dp", replicas, far)
        parts = [(0, update), (far, across)]
        for base, value in ((0, update), (far, across)):
            for step in range(1, far):
                parts.append((base ^ step, swap(value, "dp", replicas, step)))
    else:
        parts = [(0, update)] + [(step, swap(update, "dp", replicas, step)) for step in range(1, replicas)]
    for step, value in parts:
        assembled = place(assembled, source(at, replicas, step), value)
    refreshed = [
        refresh(left_new[tile], left_basis[tile], right_new[tile], right_basis[tile])
        for tile in range(tiles)
    ]
    left_basis_new = jnp.stack([pair[0] for pair in refreshed])
    right_basis_new = jnp.stack([pair[1] for pair in refreshed])
    return (
        assembled,
        momentum_new,
        second_new,
        left_new,
        right_new,
        left_basis_new,
        right_basis_new,
    )


def solution(mesh):
    block = P(("dp", "mp"), None, None)
    sizes = dict(mesh.shape)

    def body(*arrays):
        return on_device(sizes, *arrays)

    return jax.shard_map(
        body,
        mesh=mesh,
        in_specs=(P("dp", None, "mp"),) + (block,) * 6,
        out_specs=(P(None, "mp"),) + (block,) * 6,
        check_vma=False,
    )
```

```python
import jax
import jax.numpy as jnp
from jax import lax
from jax.experimental import pallas as pl
from jax.experimental.pallas import tpu as pltpu
from jax.sharding import PartitionSpec as P


beta_first = 0.9
beta_second = 0.95
epsilon = 1e-08
highest = lax.Precision.HIGHEST
SUB = 8
LANES = 128
PANEL = 32
KERNEL_BYTES = 16 * 2**20


def dot(left, right, left_dim, right_dim):
    return lax.dot_general(
        left,
        right,
        (((left_dim,), (right_dim,)), ((), ())),
        precision=highest,
        preferred_element_type=jnp.float32,
    )


def split(value):
    high = value.astype(jnp.bfloat16)
    rest = value - high.astype(jnp.float32)
    middle = rest.astype(jnp.bfloat16)
    low = (rest - middle.astype(jnp.float32)).astype(jnp.bfloat16)
    return high, middle, low


def lane(value, at):
    return jnp.broadcast_to(value[:, at:at + 1], (SUB, LANES))


def row(value, at):
    return jnp.broadcast_to(value[at:at + 1, :], (SUB, LANES))


def eliminate(work, order, rows):
    tiles = 2 * order // LANES
    groups = PANEL // SUB
    for start in range(0, order, PANEL):
        first = start // LANES
        live = range(first, tiles)
        held = [
            {v: work[start + SUB * h:start + SUB * (h + 1), v * LANES:(v + 1) * LANES] for v in live}
            for h in range(groups)
        ]
        for g in range(groups):
            at = (start + SUB * g) % LANES
            cols = {h: [lane(held[h][first], at + k) for k in range(SUB)] for h in range(g, groups)}
            yield
            for k in range(SUB):
                inverse = lax.rsqrt(row(cols[g][k], k))
                factor = {h: cols[h][k] * inverse for h in range(g, groups)}
                below = jnp.where(rows > k, factor[g], 0.0)
                for l in range(k + 1, SUB):
                    pivot = row(factor[g], l)
                    cols[g][l] = cols[g][l] - below * pivot
                    for h in range(g + 1, groups):
                        cols[h][l] = cols[h][l] - factor[h] * pivot
                for v in live:
                    top = row(held[g][v], k) * inverse
                    held[g][v] = jnp.where(rows == k, top, held[g][v] - below * top)
                    for h in range(g + 1, groups):
                        held[h][v] = held[h][v] - factor[h] * top
                yield
        for h in range(groups):
            for v in live:
                work[start + SUB * h:start + SUB * (h + 1), v * LANES:(v + 1) * LANES] = held[h][v]
        after = start + PANEL
        if after < order:
            base = (after // LANES) * LANES
            high, middle, low = split(work[start:after, base:])
            left = jnp.concatenate([high, high, middle, high, low, middle], axis=0)[:, :order - base]
            right = jnp.concatenate([high, middle, high, low, high, middle], axis=0)
            change = lax.dot_general(
                left, right, (((0,), (0,)), ((), ())), preferred_element_type=jnp.float32
            )
            work[after:, base:] = work[after:, base:] - change[after - base:]
        yield


def in_vmem(value):
    return pltpu.with_memory_space_constraint(value, pltpu.VMEM)


def local_call(body, outs, args, flops, scratch=()):
    whole = pl.BlockSpec(memory_space=pltpu.VMEM)
    return pl.pallas_call(
        body,
        out_shape=tuple(pltpu.VMEM(shape, dtype) for shape, dtype in outs),
        in_specs=[whole] * len(args),
        out_specs=(whole,) * len(outs),
        scratch_shapes=list(scratch),
        cost_estimate=pl.CostEstimate(flops=flops, transcendentals=0, bytes_accessed=0),
        compiler_params=pltpu.CompilerParams(vmem_limit_bytes=KERNEL_BYTES),
    )(*[in_vmem(value) for value in args])


def total(refs):
    value = refs[0][0].astype(jnp.float32)
    for ref in refs[1:]:
        value = value + ref[0].astype(jnp.float32)
    return value


def add_pieces(pieces):
    def body(*refs):
        refs[-1][0] = total(refs[:-1])

    return local_call(body, [(pieces[0].shape, jnp.float32)], pieces, 10**6)[0]


def square_sum(value):
    return jnp.sum(value * value, axis=0, keepdims=True)


def rotate(pieces, momentum, second, left_basis, right_basis):
    count = len(pieces)

    def body(*refs):
        momentum_ref, second_ref, left_ref, right_ref = refs[count:count + 4]
        grad_out, momentum_out, second_out, direction_out, norm_out = refs[count + 4:]
        order = left_ref.shape[1]
        gradient = total(refs[:count])
        grad_out[0] = gradient
        moment = beta_first * momentum_ref[0] + (1.0 - beta_first) * gradient
        momentum_out[0] = moment
        right = right_ref[0]
        turned = dot(left_ref[0], jnp.concatenate([gradient, moment], axis=1), 0, 0)
        grad_rot = dot(turned[:, :order], right, 1, 0)
        moment_rot = dot(turned[:, order:], right, 1, 0)
        second_new = beta_second * second_ref[0] + (1.0 - beta_second) * grad_rot * grad_rot
        second_out[0] = second_new
        direction = moment_rot / (jnp.sqrt(second_new) + epsilon)
        direction_out[0] = direction
        sums = jnp.concatenate([square_sum(gradient), square_sum(direction)], axis=0)
        norm_out[...] = jnp.broadcast_to(jnp.sum(sums, axis=1, keepdims=True), norm_out.shape)

    whole = (momentum.shape, jnp.float32)
    return local_call(
        body, [whole] * 4 + [((2, LANES), jnp.float32)],
        [*pieces, momentum, second, left_basis, right_basis], 3 * 10**8,
    )


def rotate_back(direction, left_basis, right_basis):
    def body(direction_ref, left_ref, right_ref, out):
        out[0] = dot(dot(left_ref[0], direction_ref[0], 1, 0), right_ref[0], 1, 1)

    return local_call(
        body, [(direction.shape, jnp.float32)],
        [direction, left_basis, right_basis], 10**8,
    )[0]


def scale_steps(norms, steps):
    def body(norm_ref, *refs):
        norm = norm_ref[...]
        factor = jnp.sqrt(norm[0:1, :] / norm[1:2, :])
        for at, ref in enumerate(refs[:-1]):
            for tile in range(0, ref.shape[2], LANES):
                part = ref[0, :, tile:tile + LANES] * factor
                refs[-1][at, :, tile:tile + LANES] = part.astype(jnp.bfloat16)

    shape = (len(steps),) + steps[0].shape[1:]
    return local_call(body, [(shape, jnp.bfloat16)], [norms, *steps], 10**6)[0]


def refresh_body(grad_ref, momentum_ref, second_ref, left_stat, left_basis, right_stat, right_basis,
                 momentum_out, second_out, left_out, right_out, left_basis_out, right_basis_out,
                 left_new, right_new, left_turned, right_turned, left_work, right_work, sems):
    order = left_stat.shape[1]
    rows = lax.broadcasted_iota(jnp.int32, (SUB, LANES), 0)
    copies = []

    def write(source, target):
        copies.append(pltpu.make_async_copy(source, target, sems.at[len(copies)]))
        copies[-1].start()

    write(momentum_ref, momentum_out)
    write(second_ref, second_out)
    gradient = grad_ref[0]
    left_new[0] = beta_second * left_stat[0] + (1.0 - beta_second) * dot(gradient, gradient, 1, 1)
    write(left_new, left_out)
    right_new[0] = beta_second * right_stat[0] + (1.0 - beta_second) * dot(gradient, gradient, 0, 0)
    write(right_new, right_out)
    for stat, basis, work in ((left_new, left_basis, left_work), (right_new, right_basis, right_work)):
        powered_t = dot(basis[0], stat[0], 0, 0)
        work[:, order:] = powered_t
        work[:, :order] = dot(powered_t, powered_t, 1, 1)
    for _ in zip(eliminate(left_work, order, rows), eliminate(right_work, order, rows)):
        pass
    left_turned[0] = left_work[:, order:].T
    write(left_turned, left_basis_out)
    right_turned[0] = right_work[:, order:].T
    write(right_turned, right_basis_out)
    for copy in copies:
        copy.wait()


def refresh(gradient, momentum_new, second_new, left_stat, left_basis, right_stat, right_basis):
    shape = left_stat.shape
    order = shape[-1]
    args = [gradient, momentum_new, second_new, left_stat, left_basis, right_stat, right_basis]
    block = pltpu.VMEM(shape, jnp.float32)
    work = pltpu.VMEM((order, 2 * order), jnp.float32)
    return pl.pallas_call(
        refresh_body,
        out_shape=(jax.ShapeDtypeStruct(shape, jnp.float32),) * 6,
        in_specs=[pl.BlockSpec(memory_space=pltpu.VMEM)] * len(args),
        out_specs=(pl.BlockSpec(memory_space=pl.ANY),) * 6,
        scratch_shapes=[block] * 4 + [work] * 2 + [pltpu.SemaphoreType.DMA((6,))],
        cost_estimate=pl.CostEstimate(flops=2 * 10**9, transcendentals=0, bytes_accessed=0),
        compiler_params=pltpu.CompilerParams(vmem_limit_bytes=KERNEL_BYTES),
        name="refresh",
    )(*[in_vmem(value) for value in args])


def assemble(at, gathered, far, row_count, shard_width):
    order = gathered[0][1].shape[-1]
    col_bands = shard_width // order
    steps = [step for step, _ in gathered]

    def body(at_ref, *refs):
        out, sems = refs[-2:]
        copies = []
        for step, ref in zip(steps, refs):
            for place in range(2):
                number = at_ref[0] ^ (step ^ (place * far))
                band = lax.div(number, jnp.int32(col_bands))
                top = pl.multiple_of(band * order, order)
                edge = pl.multiple_of((number - band * col_bands) * order, order)
                copies.append(pltpu.make_async_copy(
                    ref.at[place],
                    out.at[pl.ds(top, order), pl.ds(edge, order)],
                    sems.at[len(copies)],
                ))
                copies[-1].start()
        for copy in copies:
            copy.wait()

    whole = pl.BlockSpec(memory_space=pltpu.VMEM)
    return pl.pallas_call(
        body,
        out_shape=jax.ShapeDtypeStruct((row_count, shard_width), jnp.bfloat16),
        in_specs=[pl.BlockSpec(memory_space=pltpu.SMEM)] + [whole] * len(gathered),
        out_specs=pl.BlockSpec(memory_space=pl.ANY),
        scratch_shapes=[pltpu.SemaphoreType.DMA((2 * len(gathered),))],
        cost_estimate=pl.CostEstimate(flops=10**6, transcendentals=0, bytes_accessed=0),
        compiler_params=pltpu.CompilerParams(vmem_limit_bytes=KERNEL_BYTES),
        name="assemble",
    )(jnp.reshape(at, (1,)), *[in_vmem(value) for _, value in gathered])


def swap(value, axis, size, step):
    pairs = [(at, at ^ step) for at in range(size)]
    return lax.ppermute(value, axis, pairs)


def all_sum(value, sizes):
    for axis in sizes:
        step = 1
        while step < sizes[axis]:
            value = value + swap(value, axis, sizes[axis], step)
            step *= 2
    return value


def on_device(sizes, partials, momentum, second, left_stat, right_stat, left_basis, right_basis):
    order = left_basis.shape[1]
    replicas = sizes["dp"]
    far = replicas // 2
    near = range(1, far)
    at = lax.axis_index("dp")
    replica_part = partials[0]
    row_count, shard_width = replica_part.shape
    col_bands = shard_width // order

    def corner(number):
        row_band = lax.div(number, jnp.int32(col_bands))
        return row_band * order, (number - row_band * col_bands) * order

    def chunk(step):
        return lax.dynamic_slice(source, corner(at ^ step), (order, order))[None]

    source = replica_part

    first = [swap(chunk(far ^ step), "dp", replicas, step) for step in near]
    source = lax.optimization_barrier(replica_part)
    half = add_pieces([chunk(far)] + first)
    across = swap(half, "dp", replicas, far)
    second_hop = [swap(chunk(step), "dp", replicas, step) for step in near]
    gradient, momentum_new, second_new, direction, norm_local = rotate(
        [chunk(0)] + second_hop + [across], momentum, second, left_basis, right_basis
    )
    norms = all_sum(norm_local, sizes)
    raw_step = rotate_back(direction, left_basis, right_basis)
    raw_across = swap(raw_step, "dp", replicas, far)
    pair = scale_steps(norms, [raw_step, raw_across])
    gathered = [(0, pair)] + [(step, swap(pair, "dp", replicas, step)) for step in near]
    assembled = assemble(at, gathered, far, row_count, shard_width)
    momentum_new, second_new, left_new, right_new, left_basis_new, right_basis_new = refresh(
        gradient, momentum_new, second_new, left_stat, left_basis, right_stat, right_basis
    )
    return (
        assembled,
        momentum_new,
        second_new,
        left_new,
        right_new,
        left_basis_new,
        right_basis_new,
    )


def solution(mesh):
    block = P(("dp", "mp"), None, None)
    sizes = dict(mesh.shape)

    def body(*arrays):
        return on_device(sizes, *arrays)

    return jax.shard_map(
        body,
        mesh=mesh,
        in_specs=(P("dp", None, "mp"),) + (block,) * 6,
        out_specs=(P(None, "mp"),) + (block,) * 6,
        check_vma=False,
    )
```

```python
import functools
import math

import jax
import jax.numpy as jnp
from jax import lax
from jax.experimental import pallas as pl
from jax.experimental.pallas import tpu as pltpu
from jax.sharding import PartitionSpec as P


beta_first = 0.9
beta_second = 0.95
epsilon = 1e-08
highest = lax.Precision.HIGHEST
SUB = 8
LANES = 128
PANEL = 32
PARTS = 1
HEAD_PANELS = 3
KERNEL_BYTES = 16 * 2**20


def dot(left, right, left_dim, right_dim):
    return lax.dot_general(
        left,
        right,
        (((left_dim,), (right_dim,)), ((), ())),
        precision=highest,
        preferred_element_type=jnp.float32,
    )


def split(value):
    high = value.astype(jnp.bfloat16)
    rest = value - high.astype(jnp.float32)
    middle = rest.astype(jnp.bfloat16)
    low = (rest - middle.astype(jnp.float32)).astype(jnp.bfloat16)
    return high, middle, low


def lane(value, at):
    return jnp.broadcast_to(value[:, at:at + 1], (SUB, LANES))


def row(value, at):
    return jnp.broadcast_to(value[at:at + 1, :], (SUB, LANES))


def eliminate(work, rows, begin, end):
    order = work.shape[0]
    tiles = 2 * order // LANES
    groups = PANEL // SUB
    for start in range(begin, end, PANEL):
        first = start // LANES
        live = range(first, tiles)
        held = [
            {v: work[start + SUB * h:start + SUB * (h + 1), v * LANES:(v + 1) * LANES] for v in live}
            for h in range(groups)
        ]
        for g in range(groups):
            at = (start + SUB * g) % LANES
            cols = {h: [lane(held[h][first], at + k) for k in range(SUB)] for h in range(g, groups)}
            yield
            for k in range(SUB):
                inverse = lax.rsqrt(row(cols[g][k], k))
                factor = {h: cols[h][k] * inverse for h in range(g, groups)}
                below = jnp.where(rows > k, factor[g], 0.0)
                for l in range(k + 1, SUB):
                    pivot = row(factor[g], l)
                    cols[g][l] = cols[g][l] - below * pivot
                    for h in range(g + 1, groups):
                        cols[h][l] = cols[h][l] - factor[h] * pivot
                for v in live:
                    top = row(held[g][v], k) * inverse
                    held[g][v] = jnp.where(rows == k, top, held[g][v] - below * top)
                    for h in range(g + 1, groups):
                        held[h][v] = held[h][v] - factor[h] * top
                yield
        for h in range(groups):
            for v in live:
                work[start + SUB * h:start + SUB * (h + 1), v * LANES:(v + 1) * LANES] = held[h][v]
        after = start + PANEL
        if after < order:
            base = (after // LANES) * LANES
            high, middle, low = split(work[start:after, base:])
            left = jnp.concatenate([high, high, middle, high, low, middle], axis=0)[:, :order - base]
            right = jnp.concatenate([high, middle, high, low, high, middle], axis=0)
            change = lax.dot_general(
                left, right, (((0,), (0,)), ((), ())), preferred_element_type=jnp.float32
            )
            work[after:, base:] = work[after:, base:] - change[after - base:]
        yield


def in_vmem(value):
    return pltpu.with_memory_space_constraint(value, pltpu.VMEM)


def local_call(body, outs, args, flops, scratch=(), aliases=None):
    whole = pl.BlockSpec(memory_space=pltpu.VMEM)
    return pl.pallas_call(
        body,
        out_shape=tuple(pltpu.VMEM(shape, dtype) for shape, dtype in outs),
        in_specs=[whole] * len(args),
        out_specs=(whole,) * len(outs),
        scratch_shapes=list(scratch),
        input_output_aliases=aliases or {},
        cost_estimate=pl.CostEstimate(flops=flops, transcendentals=0, bytes_accessed=0),
        compiler_params=pltpu.CompilerParams(vmem_limit_bytes=KERNEL_BYTES),
    )(*[in_vmem(value) for value in args])


def total(refs):
    value = refs[0][0].astype(jnp.float32)
    for ref in refs[1:]:
        value = value + ref[0].astype(jnp.float32)
    return value


def add_pieces(pieces):
    def body(*refs):
        refs[-1][0] = total(refs[:-1])

    return local_call(body, [(pieces[0].shape, jnp.float32)], pieces, 10**6)[0]


def square_sum(value):
    return jnp.sum(value * value, axis=0, keepdims=True)


def rotate(pieces, across, momentum, second, left_basis, right_basis):
    split_at = len(pieces)
    count = split_at + len(across)

    def body(*refs):
        momentum_ref, second_ref, left_ref, right_ref = refs[count:count + 4]
        grad_out, momentum_out, second_out, direction_out, norm_out = refs[count + 4:]
        order = left_ref.shape[1]
        far_sum = jnp.concatenate([ref[0] for ref in refs[split_at:count]], axis=0)
        gradient = total(refs[:split_at]) + far_sum
        grad_out[0] = gradient
        moment = beta_first * momentum_ref[0] + (1.0 - beta_first) * gradient
        momentum_out[0] = moment
        right = right_ref[0]
        turned = dot(left_ref[0], jnp.concatenate([gradient, moment], axis=1), 0, 0)
        grad_rot = dot(turned[:, :order], right, 1, 0)
        moment_rot = dot(turned[:, order:], right, 1, 0)
        second_new = beta_second * second_ref[0] + (1.0 - beta_second) * grad_rot * grad_rot
        second_out[0] = second_new
        direction = moment_rot / (jnp.sqrt(second_new) + epsilon)
        direction_out[0] = direction
        sums = jnp.concatenate([square_sum(gradient), square_sum(direction)], axis=0)
        norm_out[...] = jnp.broadcast_to(jnp.sum(sums, axis=1, keepdims=True), norm_out.shape)

    whole = (momentum.shape, jnp.float32)
    return local_call(
        body, [whole] * 4 + [((2, LANES), jnp.float32)],
        [*pieces, *across, momentum, second, left_basis, right_basis], 3 * 10**8,
    )


def rotate_back(direction, left_basis, right_basis):
    def body(direction_ref, left_ref, right_ref, out):
        out[0] = dot(dot(left_ref[0], direction_ref[0], 1, 0), right_ref[0], 1, 1)

    return local_call(
        body, [(direction.shape, jnp.float32)],
        [direction, left_basis, right_basis], 10**8,
    )[0]


def scale_steps(norms, steps):
    def body(norm_ref, *refs):
        norm = norm_ref[...]
        factor = jnp.sqrt(norm[0:1, :] / norm[1:2, :])
        for at, ref in enumerate(refs[:-1]):
            for tile in range(0, ref.shape[2], LANES):
                part = ref[0, :, tile:tile + LANES] * factor
                refs[-1][at, :, tile:tile + LANES] = part.astype(jnp.bfloat16)

    shape = (len(steps),) + steps[0].shape[1:]
    return local_call(body, [(shape, jnp.bfloat16)], [norms, *steps], 10**6)[0]


def prepare(gradient, left_stat, left_basis, right_stat, right_basis):
    def body(grad_ref, left_stat_ref, left_ref, right_stat_ref, right_ref,
             left_new, right_new, left_work, right_work):
        order = left_ref.shape[1]
        gradient = grad_ref[0]
        left_new[0] = beta_second * left_stat_ref[0] + (1.0 - beta_second) * dot(gradient, gradient, 1, 1)
        right_new[0] = beta_second * right_stat_ref[0] + (1.0 - beta_second) * dot(gradient, gradient, 0, 0)
        for stat, basis, work in ((left_new, left_ref, left_work), (right_new, right_ref, right_work)):
            powered_t = dot(basis[0], stat[0], 0, 0)
            work[:, order:] = powered_t
            work[:, :order] = dot(powered_t, powered_t, 1, 1)

    shape = left_stat.shape
    work = ((shape[-1], 2 * shape[-1]), jnp.float32)
    return local_call(
        body, [(shape, jnp.float32)] * 2 + [work] * 2,
        [gradient, left_stat, left_basis, right_stat, right_basis], 5 * 10**8,
    )


def eliminate_both(left_work, right_work, begin, end):
    rows = lax.broadcasted_iota(jnp.int32, (SUB, LANES), 0)
    for _ in zip(eliminate(left_work, rows, begin, end), eliminate(right_work, rows, begin, end)):
        pass


def begin_refresh(left_work, right_work, end):
    def body(left_in, right_in, left_out, right_out):
        eliminate_both(left_out, right_out, 0, end)

    work = (left_work.shape, jnp.float32)
    return local_call(body, [work] * 2, [left_work, right_work], 6 * 10**8, aliases={0: 0, 1: 1})


def refresh_body(begin, momentum_ref, second_ref, left_new, right_new, left_in, right_in,
                 momentum_out, second_out, left_out, right_out, left_basis_out, right_basis_out,
                 left_work, right_work, left_turned, right_turned, sems):
    order = left_new.shape[1]
    copies = []

    def write(source, target):
        copies.append(pltpu.make_async_copy(source, target, sems.at[len(copies)]))
        copies[-1].start()

    write(momentum_ref, momentum_out)
    write(second_ref, second_out)
    write(left_new, left_out)
    write(right_new, right_out)
    eliminate_both(left_work, right_work, begin, order)
    left_turned[0] = left_work[:, order:].T
    write(left_turned, left_basis_out)
    right_turned[0] = right_work[:, order:].T
    write(right_turned, right_basis_out)
    for copy in copies:
        copy.wait()


def refresh(momentum_new, second_new, left_new, right_new, left_work, right_work, begin):
    shape = left_new.shape
    args = [momentum_new, second_new, left_new, right_new, left_work, right_work]
    block = pltpu.VMEM(shape, jnp.float32)
    whole = pl.BlockSpec(memory_space=pltpu.VMEM)
    return pl.pallas_call(
        functools.partial(refresh_body, begin),
        out_shape=(jax.ShapeDtypeStruct(shape, jnp.float32),) * 6
        + (pltpu.VMEM(left_work.shape, jnp.float32),) * 2,
        in_specs=[whole] * len(args),
        out_specs=(pl.BlockSpec(memory_space=pl.ANY),) * 6 + (whole,) * 2,
        input_output_aliases={4: 6, 5: 7},
        scratch_shapes=[block] * 2 + [pltpu.SemaphoreType.DMA((6,))],
        cost_estimate=pl.CostEstimate(flops=2 * 10**9, transcendentals=0, bytes_accessed=0),
        compiler_params=pltpu.CompilerParams(vmem_limit_bytes=KERNEL_BYTES),
        name="refresh",
    )(*[in_vmem(value) for value in args])[:6]


def assemble(at, gathered, far, row_count, shard_width):
    order = gathered[0][1].shape[-1]
    col_bands = shard_width // order
    steps = [step for step, _ in gathered]

    def body(at_ref, *refs):
        out, sems = refs[-2:]
        copies = []
        for step, ref in zip(steps, refs):
            for place in range(2):
                number = at_ref[0] ^ (step ^ (place * far))
                band = lax.div(number, jnp.int32(col_bands))
                top = pl.multiple_of(band * order, order)
                edge = pl.multiple_of((number - band * col_bands) * order, order)
                copies.append(pltpu.make_async_copy(
                    ref.at[place],
                    out.at[pl.ds(top, order), pl.ds(edge, order)],
                    sems.at[len(copies)],
                ))
                copies[-1].start()
        for copy in copies:
            copy.wait()

    whole = pl.BlockSpec(memory_space=pltpu.VMEM)
    return pl.pallas_call(
        body,
        out_shape=jax.ShapeDtypeStruct((row_count, shard_width), jnp.bfloat16),
        in_specs=[pl.BlockSpec(memory_space=pltpu.SMEM)] + [whole] * len(gathered),
        out_specs=pl.BlockSpec(memory_space=pl.ANY),
        scratch_shapes=[pltpu.SemaphoreType.DMA((2 * len(gathered),))],
        cost_estimate=pl.CostEstimate(flops=10**6, transcendentals=0, bytes_accessed=0),
        compiler_params=pltpu.CompilerParams(vmem_limit_bytes=KERNEL_BYTES),
        name="assemble",
    )(jnp.reshape(at, (1,)), *[in_vmem(value) for _, value in gathered])


def swap(value, axes, size, step):
    pairs = [(at, at ^ step) for at in range(size)]
    return lax.ppermute(value, axes, pairs)


def all_sum(value, sizes):
    axes = tuple(sizes)
    count = math.prod(sizes.values())
    low = 1
    while low < count:
        paired = low > 1 and 4 * low <= count
        others = [swap(value, axes, count, times * low) for times in range(1, 4 if paired else 2)]
        value = value + others[0]
        if paired:
            value = value + (others[1] + others[2])
        low *= 4 if paired else 2
    return value


def on_device(sizes, partials, momentum, second, left_stat, right_stat, left_basis, right_basis):
    order = left_basis.shape[1]
    replicas = sizes["dp"]
    far = replicas // 2
    near = range(1, far)
    at = lax.axis_index("dp")
    replica_part = partials[0]
    row_count, shard_width = replica_part.shape
    col_bands = shard_width // order

    def corner(number):
        row_band = lax.div(number, jnp.int32(col_bands))
        return row_band * order, (number - row_band * col_bands) * order

    def chunk(source, step, part=0, parts=1):
        top, edge = corner(at ^ step)
        rows = order // parts
        return lax.dynamic_slice(source, (top + part * rows, edge), (rows, order))[None]

    first = [
        [swap(chunk(replica_part, far ^ step, part, PARTS), "dp", replicas, step) for step in near]
        for part in range(PARTS)
    ]
    source = lax.optimization_barrier(replica_part)
    across = [
        swap(add_pieces([chunk(source, far, part, PARTS)] + first[part]), "dp", replicas, far)
        for part in range(PARTS)
    ]
    second_hop = [swap(chunk(source, step), "dp", replicas, step) for step in near]
    gradient, momentum_new, second_new, direction, norm_local = rotate(
        [chunk(source, 0)] + second_hop, across, momentum, second, left_basis, right_basis
    )
    norms = all_sum(norm_local, sizes)
    raw_step = rotate_back(direction, left_basis, right_basis)
    raw_across = swap(raw_step, "dp", replicas, far)
    pair = scale_steps(norms, [raw_step, raw_across])
    gathered = [(0, pair)] + [(step, swap(pair, "dp", replicas, step)) for step in near]
    assembled = assemble(at, gathered, far, row_count, shard_width)
    left_new, right_new, left_work, right_work = prepare(
        gradient, left_stat, left_basis, right_stat, right_basis
    )
    begin = min(HEAD_PANELS * PANEL, order)
    left_work, right_work = begin_refresh(left_work, right_work, begin)
    momentum_new, second_new, left_new, right_new, left_basis_new, right_basis_new = refresh(
        momentum_new, second_new, left_new, right_new, left_work, right_work, begin
    )
    return (
        assembled,
        momentum_new,
        second_new,
        left_new,
        right_new,
        left_basis_new,
        right_basis_new,
    )


def solution(mesh):
    block = P(("dp", "mp"), None, None)
    sizes = dict(mesh.shape)

    def body(*arrays):
        return on_device(sizes, *arrays)

    return jax.shard_map(
        body,
        mesh=mesh,
        in_specs=(P("dp", None, "mp"),) + (block,) * 6,
        out_specs=(P(None, "mp"),) + (block,) * 6,
        check_vma=False,
    )
```
